32 devices in a mesh: aa: 8 (over z, y), ba: 4 (over x, core).
Axes of the slice: x: 2, y: 2, z: 4, core: 2. Of those that a mesh axis runs over, the one named last changes fastest.
Arguments:
- features: bfloat16 [65536, 256], P(('aa', 'ba')), may hold values from -6 to 6
- tile_ids: int32 [65536, 1], P(('aa', 'ba')), may hold values from 0 to 31; in each aligned block of 2048 rows (0 to 2047, 2048 to 4095, ...) at most 96 rows name the same one
- cell_ids: int32 [65536], P(('aa', 'ba')), may hold values from 0 to 8191
- spread_weight: float32 [65536], P(('aa', 'ba')), may hold values from 0.1 to 0.6
- read_weight: float32 [65536], P(('aa', 'ba')), may hold values from 0.5 to 2
- message_weight: bfloat16 [256, 256], replicated, may hold values from -0.375 to 0.375
- skip_weight: bfloat16 [256, 256], replicated, may hold values from -0.375 to 0.375
- spectral_weight: bfloat16 [16, 256, 256, 256], P('ba', 'aa'), may hold values from -1.5 to 1.5
- hidden_weight: bfloat16 [256, 256], replicated, may hold values from -0.375 to 0.375
- output_weight: bfloat16 [256, 256], replicated, may hold values from -0.75 to 0.75
Outputs:
- point_out: bfloat16 [65536, 256], P(('aa', 'ba'))
The draws below stay inside these ranges and needn't reach their ends.
Inputs may be any that keep to these rules, and one draw needn't show every extreme that they name: `tile_ids`: among the rows of one device no index appears more than 96 times, and some index appears exactly 96 times.
All inputs are finite; a program needn't handle non-finite values.
Results may differ from the reference program's by a relative error of at most 0.015.
Values may be sent and summed in bfloat16 or wider, within the bound.
A program may use at most 64 MiB of HBM per device.

```python
import math
import jax
import jax.numpy as jnp
import numpy as np
from jax import lax

C = 256
G = 64
M = 16
P_DEV = 2048
POINTS = 65536
CAP = 96
GXD = 8
GYD = 16
CELLS_DEV = 8192
N_BA = 4
DEVICES = 32


def touch_ends(values, rng, low, largest):
    extent = values.shape
    index_at = [jax.random.randint(jax.random.fold_in(rng, axis), (), 0, extent[axis]) for axis in range(len(extent))]
    values = values.at[tuple(index_at)].set(low)
    longest = extent.index(max(extent))
    index_at[longest] = (index_at[longest] + 1) % extent[longest]
    return values.at[tuple(index_at)].set(largest)


def block_scale(stream_key, shape, pieces, low, top_value):
    factor_of, own = 1.0, jax.random.fold_in(stream_key, 6)
    for axis_at, shards_of in pieces:
        steps = jnp.exp(jax.random.uniform(jax.random.fold_in(own, axis_at), (shards_of,), jnp.float32, low / len(pieces), top_value / len(pieces)))
        factor_of = factor_of * jnp.repeat(steps, shape[axis_at] // shards_of).reshape([-1 if axis == axis_at else 1 for axis in range(len(shape))])
    return factor_of


def deal_out(own_key, own, number, rows, count, top, reach, lean):
    sequence = jax.random.permutation(own_key, count)
    heavy_load, usual = shares(count, rows * top, reach, lean, True), shares(count, rows * top, reach, lean, False)
    places = jnp.arange(count)

    def named(tallies, rotation):
        used = int((tallies > 0).sum())
        fixed = max(1, used // 4)
        moved = fixed + (places - fixed + rotation * (used - fixed)) % max(1, count - fixed)
        return jnp.zeros((count,), jnp.int32).at[sequence[jnp.where(places < fixed, places, moved)]].set(jnp.asarray(tallies, jnp.int32))

    tallies = jnp.where(number % 4 == 0, named(heavy_load, number // 4), named(usual, number - number // 4 - 1))
    mixed = jax.random.permutation(jax.random.fold_in(own, 3), count)
    giver, sink = mixed[0:count // 2 * 2:2], mixed[1:count // 2 * 2:2]
    margin = jnp.minimum(tallies[giver] - 1, reach - tallies[sink]) // 2
    margin = jnp.where((giver == sequence[0]) | (sink == sequence[0]) | (tallies[sink] == 0), 0, jnp.maximum(margin, 0))
    moved = jax.random.randint(jax.random.fold_in(own, 4), (count // 2,), 0, 1 << 20) % (margin + 1)
    tallies = tallies.at[giver].add(-moved).at[sink].add(moved)
    labels = jnp.searchsorted(jnp.cumsum(tallies), jnp.arange(rows * top), side="right").astype(jnp.int32)
    grid = labels.reshape(top, rows).T
    grid = grid[jax.random.permutation(jax.random.fold_in(own, 1), rows)]
    rotation = jax.random.randint(jax.random.fold_in(own, 2), (rows, 1), 0, top)
    return jnp.take_along_axis(grid, (jnp.arange(top)[None, :] + rotation) % top, axis=1)


def shares(count, total, bound, skew, full):
    loads = [(1 << 20) // math.isqrt(grade ** skew) + 1 for grade in range(1, count + 1)]
    largest = bound if full else min(bound, max(-(-total // count), total * loads[0] // sum(loads)))
    least = 1 if total - largest >= count - 1 else 0
    holding, spare = [largest] + [least] * (count - 1), total - largest - least * (count - 1)
    while spare > 0:
        candidates = [i for i in range(1, count) if holding[i] < largest] or [i for i in range(1, count) if holding[i] < bound]
        whole, budget = sum([loads[i] for i in candidates]), spare
        for i in candidates:
            more = min(bound - holding[i], max(1, budget * loads[i] // whole), spare)
            holding[i] = holding[i] + more
            spare = spare - more
    return np.array(holding)


def bell_draw(rng, shape, spread, most, shards=(), kind=jnp.bfloat16):
    entries = jax.random.normal(rng, shape, jnp.float32) * spread
    if len(shards) > 0:
        entries = block_scale(rng, shape, shards, -0.22, 0.18) * entries
    return jnp.clip(entries, min=-most, max=most).astype(kind)


def setup_inputs(seed: int = 0) -> dict:
    splits = jax.random.split(jax.random.key(seed), 11)
    features = bell_draw(splits[0], (POINTS, C), 1.0, 6.0, ((0, 32),))
    tile_ids_keys = jax.random.split(jax.random.fold_in(splits[1], 1), POINTS // P_DEV)
    tile_ids_turns = jax.random.permutation(jax.random.fold_in(splits[1], 3), POINTS // P_DEV)
    tile_ids = jax.vmap(lambda own, number: deal_out(jax.random.fold_in(splits[1], 2), own, number, P_DEV, DEVICES, 1, CAP, 2))(tile_ids_keys, tile_ids_turns).reshape((POINTS, 1))
    cell_ids = touch_ends(jax.random.randint(splits[2], (POINTS,), 0, CELLS_DEV), jax.random.fold_in(splits[2], 1), 0, CELLS_DEV - 1).astype(jnp.int32)
    spread_weight = jnp.clip(0.1 + 0.5 * jax.random.uniform(splits[3], (POINTS,), jnp.float32) ** block_scale(splits[3], (POINTS,), ((0, 32),), -0.2, 0.2), 0.1, 0.6)
    read_weight = jnp.clip(0.5 + 1.5 * jax.random.uniform(splits[4], (POINTS,), jnp.float32) ** block_scale(splits[4], (POINTS,), ((0, 32),), -0.2, 0.2), 0.5, 2.0)
    message_weight = bell_draw(splits[5], (C, C), C ** -0.5, 0.375)
    skip_weight = bell_draw(splits[6], (C, C), C ** -0.5, 0.375)
    spectral_weight = bell_draw(splits[7], (M, M * M, C, C), (C // 16) ** -0.5, 1.5, ((0, 4), (1, 8)))
    hidden_weight = bell_draw(splits[8], (C, C), C ** -0.5, 0.375)
    output_weight = bell_draw(splits[9], (C, C), (C // 4) ** -0.5, 0.75)
    return dict(features=features, tile_ids=tile_ids, cell_ids=cell_ids, spread_weight=spread_weight, read_weight=read_weight, message_weight=message_weight, skip_weight=skip_weight, spectral_weight=spectral_weight, hidden_weight=hidden_weight, output_weight=output_weight)


def basis_table(mode_count, grid_length, positions):
    mode_index = jnp.arange(mode_count, dtype=jnp.int32)[:, None]
    half_modes = mode_count // 2
    frequency = jnp.where(mode_index < half_modes, mode_index, mode_index - half_modes + 1).astype(jnp.float32)
    phase_angle = 2.0 * math.pi * frequency * positions.astype(jnp.float32)[None, :] / grid_length
    waveform = jnp.where(mode_index < half_modes, jnp.cos(phase_angle), jnp.sin(phase_angle))
    norm_scale = jnp.where(mode_index == 0, math.sqrt(1.0 / grid_length), math.sqrt(2.0 / grid_length))
    return (waveform * norm_scale).astype(jnp.float32)

def global_cell(tiles, cells):
    grid_x = tiles // N_BA * GXD + cells // (GYD * G)
    grid_y = tiles % N_BA * GYD + cells // G % GYD
    grid_z = cells % G
    return ((grid_x * G + grid_y) * G + grid_z).astype(jnp.int32)

def reference(features, tile_ids, cell_ids, spread_weight, read_weight, message_weight, skip_weight, spectral_weight, hidden_weight, output_weight):
    highest = lax.Precision.HIGHEST
    block_count = POINTS // P_DEV
    feat_blocks = features.reshape(block_count, P_DEV, C)
    tile_blocks = tile_ids.reshape(block_count, P_DEV)
    cell_blocks = cell_ids.reshape(block_count, P_DEV)
    spread_blocks = spread_weight.reshape(block_count, P_DEV)
    read_blocks = read_weight.reshape(block_count, P_DEV)

    def spread_step(latent_sum, block):
        feat_block, tile_block, cell_block, spread_block = block
        product = jnp.dot(feat_block, message_weight, preferred_element_type=jnp.float32)
        message = (spread_block[:, None] * product).astype(jnp.bfloat16)
        latent_sum = latent_sum.at[global_cell(tile_block, cell_block)].add(message.astype(jnp.float32))
        return (latent_sum, jnp.zeros((), jnp.float32))
    latent_sum, unused = lax.scan(spread_step, jnp.zeros((G * G * G, C), jnp.float32), (feat_blocks, tile_blocks, cell_blocks, spread_blocks))
    latent = latent_sum.astype(jnp.bfloat16)
    basis = basis_table(M, G, jnp.arange(G, dtype=jnp.int32))
    cube = latent.astype(jnp.float32).reshape(G, G, G, C)
    along_z = jnp.einsum('kz,xyzc->xykc', basis, cube, precision=highest)
    along_y = jnp.einsum('jy,xykc->xjkc', basis, along_z, precision=highest)
    spectrum = jnp.einsum('ix,xjkc->jikc', basis, along_y, precision=highest)
    spectrum = spectrum.reshape(M, M * M, C).astype(jnp.bfloat16)

    def mix_row(pair):
        spec_row, weight_row = pair
        return jnp.einsum('mc,mco->mo', spec_row.astype(jnp.float32), weight_row.astype(jnp.float32), precision=highest).astype(jnp.bfloat16)
    mixed = lax.map(mix_row, (spectrum, spectral_weight))
    mixed_cube = mixed.astype(jnp.float32).reshape(M, M, M, C)
    inv_z = jnp.einsum('kz,jikc->jizc', basis, mixed_cube, precision=highest)
    inv_x = jnp.einsum('ix,jizc->jxzc', basis, inv_z, precision=highest)
    inverse = jnp.einsum('jy,jxzc->xyzc', basis, inv_x, precision=highest)
    skip = jnp.dot(latent, skip_weight, preferred_element_type=jnp.float32)
    latent_out = jax.nn.gelu(inverse.reshape(G * G * G, C) + skip).astype(jnp.bfloat16)

    def read_step(carry, block):
        tile_block, cell_block, read_block = block
        rows = latent_out[global_cell(tile_block, cell_block)]
        gathered = (read_block[:, None] * rows.astype(jnp.float32)).astype(jnp.bfloat16)
        hidden = jax.nn.gelu(jnp.dot(gathered, hidden_weight, preferred_element_type=jnp.float32)).astype(jnp.bfloat16)
        result = jnp.dot(hidden, output_weight, preferred_element_type=jnp.float32).astype(jnp.bfloat16)
        return (carry, result)
    carry_out, results = lax.scan(read_step, jnp.zeros((), jnp.float32), (tile_blocks, cell_blocks, read_blocks))
    return results.reshape(POINTS, C)
```

```python
import functools
import math

import jax
import jax.numpy as jnp
import numpy as np
from jax import lax
from jax.experimental import pallas as pl
from jax.experimental.pallas import tpu as pltpu
from jax.sharding import PartitionSpec as P

G = 64
F32 = jnp.float32
BF16 = jnp.bfloat16


def basis_np(modes, grid):
    k = np.arange(modes)[:, None]
    half = modes // 2
    freq = np.where(k < half, k, k - half + 1).astype(np.float64)
    phase = 2.0 * math.pi * freq * np.arange(grid)[None, :] / grid
    wave = np.where(k < half, np.cos(phase), np.sin(phase))
    norm = np.where(k == 0, math.sqrt(1.0 / grid), math.sqrt(2.0 / grid))
    return (wave * norm).astype(np.float32)


def split_table(table):
    high = table.astype(BF16)
    low = (table - high.astype(np.float32)).astype(BF16)
    return np.concatenate([high, low], axis=0)


def dot(a, b):
    return jnp.dot(a, b, preferred_element_type=F32)


def blocks_of(rows, want):
    return want if rows % want == 0 else rows


def pack_kernel(devices, capacity, tiles_ref, cells_ref, message_ref, rows_ref, where_ref, slots_ref, slots):
    block = rows_ref.shape[0]
    points = message_ref.shape[0]

    @pl.when(pl.program_id(0) == 0)
    def _():
        step = blocks_of(points, 256)
        upper = (
            lax.broadcasted_iota(jnp.int32, (step, step), 0)
            <= lax.broadcasted_iota(jnp.int32, (step, step), 1)
        ).astype(F32).astype(BF16)
        carry = jnp.zeros((devices, 1), F32)
        for start in range(0, points, step):
            tiles = tiles_ref[:, start : start + step]
            hot = (lax.broadcasted_iota(jnp.int32, (devices, step), 0) == tiles).astype(F32)
            counts = dot(hot.astype(BF16), upper) + carry
            rank = jnp.sum(counts * hot, axis=0, keepdims=True) - 1.0
            slots[:, start : start + step] = tiles * capacity + rank.astype(jnp.int32)
            carry = carry + jnp.sum(hot, axis=1, keepdims=True)
        slots_ref[...] = slots[...]

    own = lax.broadcasted_iota(jnp.int32, (block, points), 0) + pl.program_id(0) * block
    hot = (own == slots[...]).astype(F32).astype(BF16)
    rows_ref[...] = dot(hot, message_ref[...]).astype(BF16)
    found = dot(hot, cells_ref[...])
    where_ref[...] = found[:, 0:1] * G + found[:, 1:2] + (found[:, 2:3] - 1.0)


def pack(tiles, cells, message, devices, capacity):
    points, width = message.shape
    total = devices * capacity
    block = blocks_of(total, 256)
    return pl.pallas_call(
        functools.partial(pack_kernel, devices, capacity),
        grid=(total // block,),
        in_specs=[
            pl.BlockSpec((1, points), lambda i: (0, 0)),
            pl.BlockSpec(cells.shape, lambda i: (0, 0)),
            pl.BlockSpec((points, width), lambda i: (0, 0)),
        ],
        out_specs=[
            pl.BlockSpec((block, width), lambda i: (i, 0)),
            pl.BlockSpec((block, 1), lambda i: (i, 0)),
            pl.BlockSpec((1, points), lambda i: (0, 0)),
        ],
        out_shape=[
            jax.ShapeDtypeStruct((total, width), BF16),
            jax.ShapeDtypeStruct((total, 1), F32),
            jax.ShapeDtypeStruct((1, points), jnp.int32),
        ],
        scratch_shapes=[pltpu.VMEM((1, points), jnp.int32)],
        cost_estimate=pl.CostEstimate(
            flops=4 * total * points * width, bytes_accessed=6 * total * width, transcendentals=0
        ),
        name="pack",
    )(tiles, cells, message)


def merge_kernel(column_ref, row_ref, rows_ref, out_ref):
    same = (column_ref[...] == row_ref[...]).astype(F32).astype(BF16)
    out_ref[...] = dot(same, rows_ref[...]).astype(BF16)


def merge(where, rows):
    total, width = rows.shape
    block = blocks_of(total, 256)
    return pl.pallas_call(
        merge_kernel,
        grid=(total // block,),
        in_specs=[
            pl.BlockSpec((block, 1), lambda i: (i, 0)),
            pl.BlockSpec((1, total), lambda i: (0, 0)),
            pl.BlockSpec((total, width), lambda i: (0, 0)),
        ],
        out_specs=pl.BlockSpec((block, width), lambda i: (i, 0)),
        out_shape=jax.ShapeDtypeStruct((total, width), BF16),
        cost_estimate=pl.CostEstimate(
            flops=2 * total * total * width, bytes_accessed=4 * total * width, transcendentals=0
        ),
        name="merge",
    )(where.reshape(total, 1), where.reshape(1, total), rows)


def hot_rows(values, points):
    lane = lax.broadcasted_iota(jnp.int32, (2 * G, points), 0) % G
    return (lane == values).astype(F32).astype(BF16)


def hot_columns(values, points):
    lane = lax.broadcasted_iota(jnp.int32, (points, 2 * G), 1) % G
    return (lane == values).astype(F32).astype(BF16)


def forward_kernel(x_ref, y_ref, z_ref, tx_ref, ty_ref, tz_ref, message_ref, out_ref, plane, second):
    points = message_ref.shape[0]
    j = pl.program_id(0)

    @pl.when(j == 0)
    def _():
        plane[...] = dot(tx_ref[...], hot_rows(x_ref[...], points)) * dot(
            tz_ref[...], hot_rows(z_ref[...], points)
        )
        second[...] = dot(ty_ref[...], hot_rows(y_ref[...], points))

    scaled = (plane[...] * second[pl.ds(j, 1), :]).astype(BF16)
    result = dot(scaled, message_ref[...])
    out_ref[...] = result.reshape(out_ref.shape).astype(BF16)


def forward(x, y, z, tables, message, axis_first, modes):
    points, width = message.shape
    tx, ty, tz = tables
    pairs = tx.shape[1]
    share = pairs // axis_first
    whole = lambda shape: pl.BlockSpec(shape, lambda j: (0,) * len(shape))
    return pl.pallas_call(
        forward_kernel,
        grid=(modes,),
        in_specs=[whole((1, points))] * 3
        + [whole((pairs, 2 * G)), whole((modes, 2 * G)), whole((pairs, 2 * G)), whole((points, width))],
        out_specs=pl.BlockSpec((axis_first, 1, share, width), lambda j: (0, j, 0, 0)),
        out_shape=jax.ShapeDtypeStruct((axis_first, modes, share, width), BF16),
        scratch_shapes=[pltpu.VMEM((pairs, points), F32), pltpu.VMEM((modes, points), F32)],
        cost_estimate=pl.CostEstimate(
            flops=2 * modes * pairs * points * width,
            bytes_accessed=2 * modes * pairs * width,
            transcendentals=0,
        ),
        name="forward",
    )(x, y, z, tx.T, ty.T, tz.T, message)


def inverse_kernel(modes, x_ref, y_ref, z_ref, tx_ref, ty_ref, tz_ref, mixed_ref, out_ref):
    points, width = out_ref.shape
    pairs = tx_ref.shape[1]
    plane = dot(hot_columns(x_ref[...], points), tx_ref[...]) * dot(
        hot_columns(z_ref[...], points), tz_ref[...]
    )
    second = dot(hot_columns(y_ref[...], points), ty_ref[...])
    total = jnp.zeros((points, width), F32)
    for j in range(modes):
        part = mixed_ref[:, j]
        if part.shape[1] % 16:
            part = part.astype(F32)
        part = part.reshape(pairs, width).astype(BF16)
        total = total + dot((plane * second[:, j : j + 1]).astype(BF16), part)
    out_ref[...] = total


def inverse(x, y, z, tables, mixed):
    points = x.shape[0]
    tx, ty, tz = tables
    modes, width = mixed.shape[1], mixed.shape[3]
    pairs = tx.shape[1]
    block = blocks_of(points, 256)
    whole = lambda shape: pl.BlockSpec(shape, lambda i: (0,) * len(shape))
    column = pl.BlockSpec((block, 1), lambda i: (i, 0))
    return pl.pallas_call(
        functools.partial(inverse_kernel, modes),
        grid=(points // block,),
        in_specs=[column] * 3 + [whole(tx.shape), whole(ty.shape), whole(tz.shape), whole(mixed.shape)],
        out_specs=pl.BlockSpec((block, width), lambda i: (i, 0)),
        out_shape=jax.ShapeDtypeStruct((points, width), F32),
        cost_estimate=pl.CostEstimate(
            flops=2 * modes * pairs * points * width,
            bytes_accessed=2 * modes * pairs * width,
            transcendentals=0,
        ),
        name="inverse",
    )(x, y, z, tx, ty, tz, mixed)


def decode_kernel(slots_ref, returned_ref, inverse_ref, read_ref, skip_ref, hidden_ref, output_ref, out_ref):
    block = out_ref.shape[0]
    total = returned_ref.shape[0]
    lane = lax.broadcasted_iota(jnp.int32, (block, total), 1)
    hot = (lane == slots_ref[...]).astype(F32).astype(BF16)
    latent = dot(hot, returned_ref[...]).astype(BF16)
    latent_out = jax.nn.gelu(inverse_ref[...] + dot(latent, skip_ref[...])).astype(BF16)
    gathered = (read_ref[...] * latent_out.astype(F32)).astype(BF16)
    hidden = jax.nn.gelu(dot(gathered, hidden_ref[...])).astype(BF16)
    out_ref[...] = dot(hidden, output_ref[...]).astype(BF16)


def decode(slots, returned, inverse_values, read, skip_weight, hidden_weight, output_weight):
    points, width = inverse_values.shape
    total = returned.shape[0]
    block = blocks_of(points, 256)
    whole = lambda shape: pl.BlockSpec(shape, lambda i: (0,) * len(shape))
    column = pl.BlockSpec((block, 1), lambda i: (i, 0))
    rows = pl.BlockSpec((block, width), lambda i: (i, 0))
    return pl.pallas_call(
        decode_kernel,
        grid=(points // block,),
        in_specs=[column, whole((total, width)), rows, column] + [whole((width, width))] * 3,
        out_specs=rows,
        out_shape=jax.ShapeDtypeStruct((points, width), BF16),
        cost_estimate=pl.CostEstimate(
            flops=2 * points * total * width, bytes_accessed=4 * total * width, transcendentals=0
        ),
        name="decode",
    )(slots, returned, inverse_values, read, skip_weight, hidden_weight, output_weight)


def per_device(
    features,
    tile_ids,
    cell_ids,
    spread_weight,
    read_weight,
    message_weight,
    skip_weight,
    spectral_weight,
    hidden_weight,
    output_weight,
):
    axes = ("aa", "ba")
    points, width = features.shape
    axis_first = lax.axis_size("aa")
    axis_second = lax.axis_size("ba")
    devices = axis_first * axis_second
    capacity = 3 * points // (2 * devices)
    tile_x = G // axis_first
    tile_y = G // axis_second
    modes_y, share = spectral_weight.shape[0], spectral_weight.shape[1]
    modes = modes_y * axis_second

    basis = basis_np(modes, G)
    tx = split_table(np.repeat(basis, modes, axis=0).T)
    tz = split_table(np.tile(basis, (modes, 1)).T)
    ty = split_table(basis.T)
    tables = (jnp.asarray(tx), jnp.asarray(ty), jnp.asarray(tz))

    targets = tile_ids[:, 0]
    x = targets // axis_second * tile_x + cell_ids // (tile_y * G)
    y = targets % axis_second * tile_y + cell_ids // G % tile_y
    z = cell_ids % G

    product = dot(features, message_weight)
    message = (spread_weight[:, None] * product).astype(BF16)
    marks = jnp.stack([cell_ids // G, cell_ids % G, jnp.ones_like(cell_ids)], axis=1)
    marks = jnp.pad(marks.astype(BF16), ((0, 0), (0, 125)))
    send_rows, send_where, slots = pack(targets[None, :], marks, message, devices, capacity)
    recv_where = lax.all_to_all(
        send_where.reshape(devices, capacity), axes, split_axis=0, concat_axis=0, tiled=True
    )
    recv_rows = lax.all_to_all(send_rows, axes, split_axis=0, concat_axis=0, tiled=True)

    partial = forward(x[None, :], y[None, :], z[None, :], tables, message, axis_first, modes)
    partial = partial.reshape(devices, modes_y, share, width)
    spectrum = lax.psum_scatter(partial, axes, scatter_dimension=0, tiled=True)[0]
    mixed = jnp.einsum(
        "jmc,jmco->jmo", spectrum, spectral_weight, preferred_element_type=F32
    ).astype(BF16)
    gathered = lax.all_gather(mixed, axes, axis=0)
    gathered = gathered.reshape(axis_first, modes, share, width)

    merged = merge(recv_where, recv_rows)
    returned = lax.all_to_all(merged, axes, split_axis=0, concat_axis=0, tiled=True)
    values = inverse(x[:, None], y[:, None], z[:, None], tables, gathered)
    return decode(
        slots.reshape(points, 1), returned, values, read_weight[:, None],
        skip_weight, hidden_weight, output_weight,
    )


def solution(mesh):
    placed = (
        P(("aa", "ba"), None),
        P(("aa", "ba"), None),
        P(("aa", "ba")),
        P(("aa", "ba")),
        P(("aa", "ba")),
        P(),
        P(),
        P("ba", "aa", None, None),
        P(),
        P(),
    )
    return jax.shard_map(
        per_device, mesh=mesh, in_specs=placed, out_specs=P(("aa", "ba"), None), check_vma=False
    )
```

```python
import functools
import math

import jax
import jax.numpy as jnp
import numpy as np
from jax import lax
from jax.experimental import pallas as pl
from jax.experimental.pallas import tpu as pltpu
from jax.sharding import PartitionSpec as P

G = 64
F32 = jnp.float32
BF16 = jnp.bfloat16


def basis_np(modes, grid):
    k = np.arange(modes)[:, None]
    half = modes // 2
    freq = np.where(k < half, k, k - half + 1).astype(np.float64)
    phase = 2.0 * math.pi * freq * np.arange(grid)[None, :] / grid
    wave = np.where(k < half, np.cos(phase), np.sin(phase))
    norm = np.where(k == 0, math.sqrt(1.0 / grid), math.sqrt(2.0 / grid))
    return (wave * norm).astype(np.float32)


def split_table(table):
    high = table.astype(BF16)
    low = (table - high.astype(np.float32)).astype(BF16)
    return np.concatenate([high, low], axis=0)


def dot(a, b):
    return jnp.dot(a, b, preferred_element_type=F32)


def blocks_of(rows, want):
    return want if rows % want == 0 else rows


def pack_kernel(devices, capacity, tiles_ref, cells_ref, message_ref, rows_ref, where_ref, slots_ref, slots):
    block = rows_ref.shape[0]
    points = message_ref.shape[0]

    @pl.when(pl.program_id(0) == 0)
    def _():
        step = blocks_of(points, 256)
        upper = (
            lax.broadcasted_iota(jnp.int32, (step, step), 0)
            <= lax.broadcasted_iota(jnp.int32, (step, step), 1)
        ).astype(F32).astype(BF16)
        carry = jnp.zeros((devices, 1), F32)
        for start in range(0, points, step):
            tiles = tiles_ref[:, start : start + step]
            hot = (lax.broadcasted_iota(jnp.int32, (devices, step), 0) == tiles).astype(F32)
            counts = dot(hot.astype(BF16), upper) + carry
            rank = jnp.sum(counts * hot, axis=0, keepdims=True) - 1.0
            slots[:, start : start + step] = tiles * capacity + rank.astype(jnp.int32)
            carry = carry + jnp.sum(hot, axis=1, keepdims=True)
        slots_ref[...] = slots[...]

    own = lax.broadcasted_iota(jnp.int32, (block, points), 0) + pl.program_id(0) * block
    hot = (own == slots[...]).astype(F32).astype(BF16)
    rows_ref[...] = dot(hot, message_ref[...]).astype(BF16)
    found = dot(hot, cells_ref[...])
    where_ref[...] = found[:, 0:1] * G + found[:, 1:2] + (found[:, 2:3] - 1.0)


def pack(tiles, cells, message, devices, capacity):
    points, width = message.shape
    total = devices * capacity
    block = blocks_of(total, 256)
    return pl.pallas_call(
        functools.partial(pack_kernel, devices, capacity),
        grid=(total // block,),
        in_specs=[
            pl.BlockSpec((1, points), lambda i: (0, 0)),
            pl.BlockSpec(cells.shape, lambda i: (0, 0)),
            pl.BlockSpec((points, width), lambda i: (0, 0)),
        ],
        out_specs=[
            pl.BlockSpec((block, width), lambda i: (i, 0)),
            pl.BlockSpec((block, 1), lambda i: (i, 0)),
            pl.BlockSpec((1, points), lambda i: (0, 0)),
        ],
        out_shape=[
            jax.ShapeDtypeStruct((total, width), BF16),
            jax.ShapeDtypeStruct((total, 1), F32),
            jax.ShapeDtypeStruct((1, points), jnp.int32),
        ],
        scratch_shapes=[pltpu.VMEM((1, points), jnp.int32)],
        cost_estimate=pl.CostEstimate(
            flops=4 * total * points * width, bytes_accessed=6 * total * width, transcendentals=0
        ),
        name="pack",
    )(tiles, cells, message)


def merge_kernel(column_ref, row_ref, rows_ref, out_ref):
    same = (column_ref[...] == row_ref[...]).astype(F32).astype(BF16)
    out_ref[...] = dot(same, rows_ref[...]).astype(BF16)


def merge(where, rows):
    total, width = rows.shape
    block = blocks_of(total, 256)
    return pl.pallas_call(
        merge_kernel,
        grid=(total // block,),
        in_specs=[
            pl.BlockSpec((block, 1), lambda i: (i, 0)),
            pl.BlockSpec((1, total), lambda i: (0, 0)),
            pl.BlockSpec((total, width), lambda i: (0, 0)),
        ],
        out_specs=pl.BlockSpec((block, width), lambda i: (i, 0)),
        out_shape=jax.ShapeDtypeStruct((total, width), BF16),
        cost_estimate=pl.CostEstimate(
            flops=2 * total * total * width, bytes_accessed=4 * total * width, transcendentals=0
        ),
        name="merge",
    )(where.reshape(total, 1), where.reshape(1, total), rows)


def hot_rows(values, points):
    lane = lax.broadcasted_iota(jnp.int32, (2 * G, points), 0) % G
    return (lane == values).astype(F32).astype(BF16)


def hot_columns(values, points):
    lane = lax.broadcasted_iota(jnp.int32, (points, 2 * G), 1) % G
    return (lane == values).astype(F32).astype(BF16)


def forward_kernel(x_ref, y_ref, z_ref, tx_ref, ty_ref, tz_ref, message_ref, out_ref, plane, second):
    points = message_ref.shape[0]
    j = pl.program_id(0)

    @pl.when(j == 0)
    def _():
        plane[...] = dot(tx_ref[...], hot_rows(x_ref[...], points)) * dot(
            tz_ref[...], hot_rows(z_ref[...], points)
        )
        second[...] = dot(ty_ref[...], hot_rows(y_ref[...], points))

    scaled = (plane[...] * second[pl.ds(j, 1), :]).astype(BF16)
    result = dot(scaled, message_ref[...])
    out_ref[...] = result.reshape(out_ref.shape).astype(BF16)


def forward(x, y, z, tables, message, axis_first, modes):
    points, width = message.shape
    tx, ty, tz = tables
    pairs = tx.shape[1]
    share = pairs // axis_first
    whole = lambda shape: pl.BlockSpec(shape, lambda j: (0,) * len(shape))
    return pl.pallas_call(
        forward_kernel,
        grid=(modes,),
        in_specs=[whole((1, points))] * 3
        + [whole((pairs, 2 * G)), whole((modes, 2 * G)), whole((pairs, 2 * G)), whole((points, width))],
        out_specs=pl.BlockSpec((axis_first, 1, share, width), lambda j: (0, j, 0, 0)),
        out_shape=jax.ShapeDtypeStruct((axis_first, modes, share, width), BF16),
        scratch_shapes=[pltpu.VMEM((pairs, points), F32), pltpu.VMEM((modes, points), F32)],
        cost_estimate=pl.CostEstimate(
            flops=2 * modes * pairs * points * width,
            bytes_accessed=2 * modes * pairs * width,
            transcendentals=0,
        ),
        name="forward",
    )(x, y, z, tx.T, ty.T, tz.T, message)


def inverse_kernel(modes, x_ref, y_ref, z_ref, tx_ref, ty_ref, tz_ref, mixed_ref, out_ref):
    points, width = out_ref.shape
    pairs = tx_ref.shape[1]
    plane = dot(hot_columns(x_ref[...], points), tx_ref[...]) * dot(
        hot_columns(z_ref[...], points), tz_ref[...]
    )
    second = dot(hot_columns(y_ref[...], points), ty_ref[...])
    total = jnp.zeros((points, width), F32)
    for j in range(modes):
        part = mixed_ref[:, j]
        if part.shape[1] % 16:
            part = part.astype(F32)
        part = part.reshape(pairs, width).astype(BF16)
        total = total + dot((plane * second[:, j : j + 1]).astype(BF16), part)
    out_ref[...] = total


def inverse(x, y, z, tables, mixed):
    points = x.shape[0]
    tx, ty, tz = tables
    modes, width = mixed.shape[1], mixed.shape[3]
    pairs = tx.shape[1]
    block = blocks_of(points, 256)
    whole = lambda shape: pl.BlockSpec(shape, lambda i: (0,) * len(shape))
    column = pl.BlockSpec((block, 1), lambda i: (i, 0))
    return pl.pallas_call(
        functools.partial(inverse_kernel, modes),
        grid=(points // block,),
        in_specs=[column] * 3 + [whole(tx.shape), whole(ty.shape), whole(tz.shape), whole(mixed.shape)],
        out_specs=pl.BlockSpec((block, width), lambda i: (i, 0)),
        out_shape=jax.ShapeDtypeStruct((points, width), F32),
        cost_estimate=pl.CostEstimate(
            flops=2 * modes * pairs * points * width,
            bytes_accessed=2 * modes * pairs * width,
            transcendentals=0,
        ),
        name="inverse",
    )(x, y, z, tx, ty, tz, mixed)


def decode_kernel(slots_ref, returned_ref, inverse_ref, read_ref, skip_ref, hidden_ref, output_ref, out_ref):
    block = out_ref.shape[0]
    total = returned_ref.shape[0]
    lane = lax.broadcasted_iota(jnp.int32, (block, total), 1)
    hot = (lane == slots_ref[...]).astype(F32).astype(BF16)
    latent = dot(hot, returned_ref[...]).astype(BF16)
    latent_out = jax.nn.gelu(inverse_ref[...] + dot(latent, skip_ref[...])).astype(BF16)
    gathered = (read_ref[...] * latent_out.astype(F32)).astype(BF16)
    hidden = jax.nn.gelu(dot(gathered, hidden_ref[...])).astype(BF16)
    out_ref[...] = dot(hidden, output_ref[...]).astype(BF16)


def decode(slots, returned, inverse_values, read, skip_weight, hidden_weight, output_weight):
    points, width = inverse_values.shape
    total = returned.shape[0]
    block = blocks_of(points, 256)
    whole = lambda shape: pl.BlockSpec(shape, lambda i: (0,) * len(shape))
    column = pl.BlockSpec((block, 1), lambda i: (i, 0))
    rows = pl.BlockSpec((block, width), lambda i: (i, 0))
    return pl.pallas_call(
        decode_kernel,
        grid=(points // block,),
        in_specs=[column, whole((total, width)), rows, column] + [whole((width, width))] * 3,
        out_specs=rows,
        out_shape=jax.ShapeDtypeStruct((points, width), BF16),
        cost_estimate=pl.CostEstimate(
            flops=2 * points * total * width, bytes_accessed=4 * total * width, transcendentals=0
        ),
        name="decode",
    )(slots, returned, inverse_values, read, skip_weight, hidden_weight, output_weight)


def per_device(
    features,
    tile_ids,
    cell_ids,
    spread_weight,
    read_weight,
    message_weight,
    skip_weight,
    spectral_weight,
    hidden_weight,
    output_weight,
):
    axes = ("aa", "ba")
    points, width = features.shape
    axis_first = lax.axis_size("aa")
    axis_second = lax.axis_size("ba")
    devices = axis_first * axis_second
    capacity = 3 * points // (2 * devices)
    tile_x = G // axis_first
    tile_y = G // axis_second
    modes_y, share = spectral_weight.shape[0], spectral_weight.shape[1]
    modes = modes_y * axis_second

    basis = basis_np(modes, G)
    tx = split_table(np.repeat(basis, modes, axis=0).T)
    tz = split_table(np.tile(basis, (modes, 1)).T)
    ty = split_table(basis.T)
    tables = (jnp.asarray(tx), jnp.asarray(ty), jnp.asarray(tz))

    targets = tile_ids[:, 0]
    x = targets // axis_second * tile_x + cell_ids // (tile_y * G)
    y = targets % axis_second * tile_y + cell_ids // G % tile_y
    z = cell_ids % G

    product = dot(features, message_weight)
    message = (spread_weight[:, None] * product).astype(BF16)
    marks = jnp.stack([cell_ids // G, cell_ids % G, jnp.ones_like(cell_ids)], axis=1)
    marks = jnp.pad(marks.astype(BF16), ((0, 0), (0, 125)))
    send_rows, send_where, slots = pack(targets[None, :], marks, message, devices, capacity)
    recv_where = lax.all_to_all(
        send_where.reshape(devices, capacity), axes, split_axis=0, concat_axis=0, tiled=True
    )
    recv_rows = lax.all_to_all(send_rows, axes, split_axis=0, concat_axis=0, tiled=True)

    partial = forward(x[None, :], y[None, :], z[None, :], tables, message, axis_first, modes)
    partial = partial.reshape(devices, modes_y, share, width)
    partial = partial.reshape(axis_first, axis_second, modes_y, share, width)
    partial = lax.all_to_all(partial, 'ba', split_axis=1, concat_axis=1, tiled=True)
    partial = jnp.sum(partial.astype(F32), axis=1).astype(BF16)
    partial = lax.all_to_all(partial, 'aa', split_axis=0, concat_axis=0, tiled=True)
    spectrum = jnp.sum(partial.astype(F32), axis=0).astype(BF16)
    mixed = jnp.einsum(
        "jmc,jmco->jmo", spectrum, spectral_weight, preferred_element_type=F32
    ).astype(BF16)
    gathered = lax.all_gather(mixed, 'ba', axis=0, tiled=True)
    gathered = lax.all_gather(gathered, 'aa', axis=0)

    merged = merge(recv_where, recv_rows)
    returned = lax.all_to_all(merged, axes, split_axis=0, concat_axis=0, tiled=True)
    values = inverse(x[:, None], y[:, None], z[:, None], tables, gathered)
    return decode(
        slots.reshape(points, 1), returned, values, read_weight[:, None],
        skip_weight, hidden_weight, output_weight,
    )


def solution(mesh):
    placed = (
        P(("aa", "ba"), None),
        P(("aa", "ba"), None),
        P(("aa", "ba")),
        P(("aa", "ba")),
        P(("aa", "ba")),
        P(),
        P(),
        P("ba", "aa", None, None),
        P(),
        P(),
    )
    return jax.shard_map(
        per_device, mesh=mesh, in_specs=placed, out_specs=P(("aa", "ba"), None), check_vma=False
    )
```
